32 devices in a mesh: heads: 4 (over x, core), ctx: 8 (over z, y).
Axes of the slice: x: 2, y: 2, z: 4, core: 2. Of those that a mesh axis runs over, the one named last changes fastest.
Arguments:
- queries: bfloat16 [1536, 2048], P('ctx', 'heads'), may hold values from -6 to 6
- key_states: bfloat16 [1536, 512], P('ctx', 'heads'), may hold values from -6 to 6
- value_states: bfloat16 [1536, 512], P('ctx', 'heads'), may hold values from -6 to 6
- attention_out: bfloat16 [1536, 2048], P('ctx', 'heads'), may hold values from -2 to 2
- out_grad: bfloat16 [1536, 2048], P('ctx', 'heads'), may hold values from -6 to 6
- log_sum_exp: float32 [16, 1536], P('heads', 'ctx'), may hold values from 0 to 16, as said below
- block_counts: int32 [8], replicated, may hold values from 1 to 3, as said below
- w_query: bfloat16 [4096, 2048], P(None, 'heads'), may hold values from -0.09375 to 0.09375
- w_key: bfloat16 [4096, 512], P(None, 'heads'), may hold values from -0.09375 to 0.09375
- w_value: bfloat16 [4096, 512], P(None, 'heads'), may hold values from -0.09375 to 0.09375
Outputs:
- input_grad: bfloat16 [1536, 4096], P('ctx', 'heads')
- key_grad: float32 [1536, 512], P('ctx', 'heads')
- value_grad: float32 [1536, 512], P('ctx', 'heads')
The draws below stay inside these ranges and needn't reach their ends.
Inputs may be any that keep to these rules, and one draw needn't show every extreme that they name: `block_counts`: one entry equals 3. `log_sum_exp`: finite offsets of each row's scores.
All inputs are finite; a program needn't handle non-finite values.
Results may differ from the reference program's by a relative error of at most 0.0063.
Values may be sent and summed in bfloat16 or wider, within the bound.
A program may use at most 128 MiB of HBM per device.

```python
import math
import jax
import jax.numpy as jnp
from jax import lax

D_MODEL = 4096
HEAD_DIM = 128
GROUP = 4
CAP = 192
BLOCK = 64
KV_HEADS = 4
TOKENS_CAP = 1536
N_CTX = 8


def shared_counts(key):
    count_key = jax.random.fold_in(key, 101)
    pick_key = jax.random.fold_in(key, 202)
    counts = jax.random.randint(count_key, (N_CTX,), 1, CAP // BLOCK + 1, dtype=jnp.int32)
    chosen = jax.random.randint(pick_key, (), 0, N_CTX, dtype=jnp.int32)
    return jnp.where(jnp.arange(N_CTX, dtype=jnp.int32) == chosen, CAP // BLOCK, counts).astype(jnp.int32)


def draw_block_counts(key, part):
    return shared_counts(key)


def draw_log_sum_exp(key, part):
    counts = shared_counts(key)
    lengths = counts * BLOCK
    offsets = jnp.cumsum(lengths) - lengths
    row_index = jnp.arange(CAP * N_CTX, dtype=jnp.int32)
    device = row_index // CAP
    within = row_index - device * CAP
    position = offsets[device] + within
    visible_keys = (position + 1).astype(jnp.float32)
    noise_key = jax.random.fold_in(key, 303)
    base = jax.random.uniform(noise_key, (KV_HEADS * GROUP, CAP * N_CTX), jnp.float32, 0.3, 1.2)
    return jnp.log(visible_keys)[None, :] + base


def steps_of(rng, shape, split, least, high):
    level = 1.0
    for dim, blocks in split:
        steps = jax.random.uniform(jax.random.fold_in(jax.random.fold_in(rng, 6), dim), (blocks,), jnp.float32, least / len(split), high / len(split))
        level = level * jnp.repeat(jnp.exp(steps), shape[dim] // blocks).reshape((-1,) + (1,) * (len(shape) - 1 - dim))
    return level


def bell_draw(rng, shape, spread, reach, pieces=(), held_as=jnp.bfloat16):
    entries = jax.random.normal(rng, shape, jnp.float32) * spread
    if len(pieces) > 0:
        entries = steps_of(rng, shape, pieces, -0.22, 0.18) * entries
    return jnp.clip(entries, min=-reach, max=reach).astype(held_as)


def setup_inputs(seed: int = 0) -> dict:
    splits = jax.random.split(jax.random.key(seed), 11)
    queries = bell_draw(splits[0], (TOKENS_CAP, KV_HEADS * GROUP * HEAD_DIM), 1.0, 6.0, ((0, 8), (1, 4)))
    key_states = bell_draw(splits[1], (TOKENS_CAP, KV_HEADS * HEAD_DIM), 1.0, 6.0, ((0, 8), (1, 4)))
    value_states = bell_draw(splits[2], (TOKENS_CAP, KV_HEADS * HEAD_DIM), 1.0, 6.0, ((0, 8), (1, 4)))
    attention_out = bell_draw(splits[3], (TOKENS_CAP, KV_HEADS * GROUP * HEAD_DIM), 0.3, 2.0, ((0, 8), (1, 4)))
    out_grad = bell_draw(splits[4], (TOKENS_CAP, KV_HEADS * GROUP * HEAD_DIM), 1.0, 6.0, ((0, 8), (1, 4)))
    log_sum_exp = draw_log_sum_exp(jax.random.fold_in(splits[10], 71), 0)
    block_counts = draw_block_counts(jax.random.fold_in(splits[10], 71), 0)
    w_query = bell_draw(splits[7], (D_MODEL, KV_HEADS * GROUP * HEAD_DIM), D_MODEL ** -0.5, 0.09375, ((1, 4),))
    w_key = bell_draw(splits[8], (D_MODEL, KV_HEADS * HEAD_DIM), D_MODEL ** -0.5, 0.09375, ((1, 4),))
    w_value = bell_draw(splits[9], (D_MODEL, KV_HEADS * HEAD_DIM), D_MODEL ** -0.5, 0.09375, ((1, 4),))
    return dict(queries=queries, key_states=key_states, value_states=value_states, attention_out=attention_out, out_grad=out_grad, log_sum_exp=log_sum_exp, block_counts=block_counts, w_query=w_query, w_key=w_key, w_value=w_value)


def slot_table(block_counts):
    lengths = (block_counts * BLOCK).astype(jnp.int32)
    offsets = (jnp.cumsum(lengths) - lengths).astype(jnp.int32)
    row_index = jnp.arange(CAP * N_CTX, dtype=jnp.int32)
    device = row_index // CAP
    within = row_index - device * CAP
    position = offsets[device] + within
    live = within < lengths[device]
    return (position, live)

def reference(queries, key_states, value_states, attention_out, out_grad, log_sum_exp, block_counts, w_query, w_key, w_value):
    total_rows = CAP * N_CTX
    score_scale = 1.0 / math.sqrt(HEAD_DIM)
    position, live = slot_table(block_counts)
    query_block = math.gcd(total_rows, 512)
    width = GROUP * HEAD_DIM
    query_parts = []
    key_parts = []
    value_parts = []
    for head_num in range(KV_HEADS):
        query_h = queries[:, head_num * width:(head_num + 1) * width].reshape(total_rows, GROUP, HEAD_DIM)
        grad_h = out_grad[:, head_num * width:(head_num + 1) * width].reshape(total_rows, GROUP, HEAD_DIM)
        output_h = attention_out[:, head_num * width:(head_num + 1) * width].reshape(total_rows, GROUP, HEAD_DIM)
        key_h = key_states[:, head_num * HEAD_DIM:(head_num + 1) * HEAD_DIM].astype(jnp.float32)
        value_h = value_states[:, head_num * HEAD_DIM:(head_num + 1) * HEAD_DIM].astype(jnp.float32)
        norm_h = log_sum_exp[head_num * GROUP:(head_num + 1) * GROUP]
        delta_h = lax.optimization_barrier(jnp.sum(grad_h.astype(jnp.float32) * output_h.astype(jnp.float32), axis=2))

        def step_block(totals, block_num):
            key_acc, value_acc = totals
            begin_row = (block_num * query_block).astype(jnp.int32)
            query_blk = lax.dynamic_slice_in_dim(query_h, begin_row, query_block, 0).astype(jnp.float32)
            grad_blk = lax.dynamic_slice_in_dim(grad_h, begin_row, query_block, 0).astype(jnp.float32)
            norm_blk = lax.dynamic_slice_in_dim(norm_h, begin_row, query_block, 1)
            delta_blk = lax.dynamic_slice_in_dim(delta_h, begin_row, query_block, 0)
            query_pos = lax.dynamic_slice_in_dim(position, begin_row, query_block, 0)
            query_live = lax.dynamic_slice_in_dim(live, begin_row, query_block, 0)
            scores = jnp.einsum('qgd,kd->gqk', query_blk, key_h) * score_scale
            visible = query_live[:, None] & live[None, :] & (position[None, :] <= query_pos[:, None])
            probability = jnp.where(visible[None], jnp.exp(scores - norm_blk[:, :, None]), 0.0)
            prob_grad = jnp.einsum('qgd,kd->gqk', grad_blk, value_h)
            score_grad = probability * (prob_grad - delta_blk.T[:, :, None])
            prob_b = probability.astype(jnp.bfloat16).astype(jnp.float32)
            grad_b = score_grad.astype(jnp.bfloat16).astype(jnp.float32)
            query_terms = score_scale * jnp.einsum('gqk,kd->qgd', grad_b, key_h)
            key_acc = key_acc + score_scale * jnp.einsum('gqk,qgd->kd', grad_b, query_blk)
            value_acc = value_acc + jnp.einsum('gqk,qgd->kd', prob_b, grad_blk)
            return ((key_acc, value_acc), query_terms)
        zero_keys = jnp.zeros((total_rows, HEAD_DIM), jnp.float32)
        (key_acc, value_acc), grad_blocks = lax.scan(step_block, (zero_keys, zero_keys), jnp.arange(total_rows // query_block, dtype=jnp.int32))
        query_parts.append(grad_blocks.reshape(total_rows, width))
        key_parts.append(key_acc)
        value_parts.append(value_acc)
    query_grad = jnp.concatenate(query_parts, axis=1)
    key_grad = jnp.concatenate(key_parts, axis=1)
    value_grad = jnp.concatenate(value_parts, axis=1)
    input_grad = jnp.dot(query_grad.astype(jnp.bfloat16), w_query.T, preferred_element_type=jnp.float32)
    input_grad = input_grad + jnp.dot(key_grad.astype(jnp.bfloat16), w_key.T, preferred_element_type=jnp.float32)
    input_grad = input_grad + jnp.dot(value_grad.astype(jnp.bfloat16), w_value.T, preferred_element_type=jnp.float32)
    return (input_grad.astype(jnp.bfloat16), key_grad, value_grad)
```

```python
import functools
import math

import jax
import jax.numpy as jnp
from jax import lax
from jax.experimental import pallas as pl
from jax.experimental.pallas import tpu as pltpu
from jax.sharding import PartitionSpec as P

BLOCK = 64
LOG2E = math.log2(math.e)
F32 = jnp.float32
BF16 = jnp.bfloat16
NT = (((1,), (1,)), ((), ()))
TN = (((0,), (0,)), ((), ()))


def dot(a, b, dims=(((1,), (0,)), ((), ()))):
    return lax.dot_general(a, b, dims, preferred_element_type=F32)


def kernel(
    zs, nx, ns,
    q_ref, k_ref, v_ref, o_ref, do_ref, lse_ref, cnt_ref, wq_hbm, wk_hbm, wv_hbm,
    out_ref, dk_ref, dv_ref,
    wq, wkv, qs, dos, lse2, delta, dqt, gq, gkv, acc, kv, part, psend, prcv, fsend, frcv,
    pre, tsend, trcv, xsend, xrcv,
    w_sem, own_send, pair_send, rel_send, kv_recv, p_send, p_recv, f_send, f_recv,
    t_send, t_recv, x_send, x_recv,
):
    cap, dim = k_ref.shape
    group = q_ref.shape[1] // dim
    scale = 1.0 / math.sqrt(dim)
    me = lax.axis_index("ctx")
    y = lax.rem(me, 2)
    z = lax.div(me, 2)
    pair = me + 1 - 2 * y
    h = lax.axis_index("heads")
    core = lax.rem(h, 2)
    x = lax.div(h, 2)
    other = h + 1 - 2 * core
    across = [2 * lax.rem(x + dx, nx) + core for dx in range(nx)]

    w_copies = [
        pltpu.make_async_copy(wq_hbm, wq, w_sem.at[0]),
        pltpu.make_async_copy(wk_hbm, wkv.at[:, pl.ds(0, dim)], w_sem.at[1]),
        pltpu.make_async_copy(wv_hbm, wkv.at[:, pl.ds(dim, dim)], w_sem.at[2]),
    ]

    def remote(src, dst, send, recv, **device):
        return pltpu.make_async_remote_copy(
            src_ref=src, dst_ref=dst, send_sem=send, recv_sem=recv,
            device_id=device, device_id_type=pl.DeviceIdType.MESH,
        )

    barrier = pltpu.get_barrier_semaphore()

    def greet(**device):
        pl.semaphore_signal(
            barrier, inc=1, device_id=device, device_id_type=pl.DeviceIdType.MESH
        )

    def greet_line(z2, _):
        @pl.when(z2 != z)
        def _():
            greet(ctx=2 * z2 + y)
        return 0

    lax.fori_loop(0, zs, greet_line, 0)
    greet(ctx=pair)
    greet(heads=other)
    for dx in range(1, nx):
        greet(heads=across[dx])
    for copy in w_copies:
        copy.start()
    pl.semaphore_wait(barrier, zs + nx)

    own = (k_ref, v_ref)

    def own_copy(t, z2):
        return remote(own[t], kv.at[t, me], own_send.at[t, z2], kv_recv.at[t, me], ctx=2 * z2 + y)

    def pair_copy(t):
        return remote(own[t], kv.at[t, me], pair_send.at[t], kv_recv.at[t, me], ctx=pair)

    def relay_copy(t, z1):
        b = 2 * z1 + y
        return remote(kv.at[t, b], kv.at[t, b], rel_send.at[t, z1], kv_recv.at[t, b], ctx=pair)

    def arrived(b):
        for t in range(2):
            remote(kv.at[t, b], kv.at[t, b], pair_send.at[t], kv_recv.at[t, b], ctx=pair).wait_recv()

    def part_copy(z1):
        return remote(psend.at[z1], prcv.at[z1], p_send.at[z1], p_recv.at[z1], ctx=pair)

    def fin_copy(z1):
        return remote(fsend.at[z1], frcv.at[z], f_send.at[z1], f_recv.at[z], ctx=2 * z1 + y)

    def fin_wait(z2):
        remote(fsend.at[z2], frcv.at[z2], f_send.at[z2], f_recv.at[z2], ctx=2 * z2 + y).wait_recv()

    @pl.when(y == 0)
    def _():
        for t in range(2):
            pair_copy(t).start()

    def push_own(i, _):
        z2 = zs - 1 - i

        @pl.when(z2 > z)
        def _():
            for t in range(2):
                own_copy(t, z2).start()
        return 0

    lax.fori_loop(0, zs, push_own, 0)

    ones = jnp.ones((8, dim), F32)
    lane = lax.broadcasted_iota(jnp.int32, (1, group * cap), 1)
    row = lax.rem(lane, cap)
    alive = row < cnt_ref[me] * BLOCK
    for g in range(group):
        cols = slice(g * dim, (g + 1) * dim)
        qs[g * cap:(g + 1) * cap, :] = q_ref[:, cols]
        dos[g * cap:(g + 1) * cap, :] = do_ref[:, cols]
    prod = jnp.concatenate(
        [
            do_ref[:, g * dim:(g + 1) * dim].astype(F32) * o_ref[:, g * dim:(g + 1) * dim].astype(F32)
            for g in range(group)
        ],
        axis=0,
    )
    delta[...] = lax.dot_general(
        ones, prod, NT, preferred_element_type=F32, precision=lax.Precision.HIGHEST
    )[0:1]
    lse_row = jnp.concatenate([lse_ref[g:g + 1, :] for g in range(group)], axis=1)
    lse2[...] = jnp.where(alive, lse_row * LOG2E, 1e30)

    key_row = lax.broadcasted_iota(jnp.int32, (cap, group * cap), 0)

    def tile(key, value, b, diagonal):
        scores = dot(key, qs[...], NT)
        prob_grad = dot(value, dos[...], NT)
        visible = key_row < cnt_ref[b] * BLOCK
        if diagonal:
            visible = visible & (key_row <= row)
        prob = jnp.where(visible, jnp.exp2(scores * (scale * LOG2E) - lse2[...]), 0.0)
        grad = (prob * (prob_grad - delta[...])).astype(BF16)
        d_value = dot(prob.astype(BF16), dos[...])
        d_key = dot(grad, qs[...])
        terms = dot(key, grad, TN)
        if diagonal:
            dqt[...] = terms
        else:
            dqt[...] += terms
        return d_key, d_value

    d_key, d_value = tile(k_ref[...], v_ref[...], me, True)
    acc[0] = d_key
    acc[1] = d_value

    def pair_tile(z1):
        b = 2 * z1 + 1 - y
        arrived(b)
        d_key, d_value = tile(kv[0, b], kv[1, b], b, False)
        psend[z1, 0] = d_key.astype(BF16)
        psend[z1, 1] = d_value.astype(BF16)
        part_copy(z1).start()

    def combine(z1):
        part_copy(z1).wait_recv()
        fsend[z1] = (part[z1] + prcv[z1].astype(F32)).astype(BF16)
        fin_copy(z1).start()

    def step(i, _):
        z1 = z - i

        @pl.when((z1 >= 0) & (i > 0))
        def _():
            b = 2 * z1 + y
            arrived(b)
            for t in range(2):
                relay_copy(t, z1).start()
            d_key, d_value = tile(kv[0, b], kv[1, b], b, False)
            part[z1, 0] = d_key
            part[z1, 1] = d_value

        @pl.when((z1 >= 0) & ((i > 0) | (y == 1)))
        def _():
            pair_tile(z1)

        @pl.when((z1 >= -1) & (i > 1))
        def _():
            combine(z1 + 1)
        return 0

    lax.fori_loop(0, zs + 1, step, 0)

    query_grad = (jnp.transpose(dqt[...]) * scale).astype(BF16)
    for g in range(group):
        gq[:, g * dim:(g + 1) * dim] = query_grad[g * cap:(g + 1) * cap, :]
    for copy in w_copies:
        copy.wait()
    width = pre.shape[2]

    def project(i, _):
        pre[i] = dot(gq[...], wq[pl.ds(pl.multiple_of(i * width, width), width), :], NT)
        return 0

    lax.fori_loop(0, pre.shape[0], project, 0)

    @pl.when(y == 0)
    def _():
        part_copy(z).wait_recv()
        acc[...] += prcv[z].astype(F32)

    def collect(z2, _):
        @pl.when(z2 > z)
        def _():
            fin_wait(z2)
            acc[...] += frcv[z2].astype(F32)
        return 0

    lax.fori_loop(0, zs, collect, 0)
    key_total = acc[0] * scale
    value_total = acc[1]
    dk_ref[...] = key_total
    dv_ref[...] = value_total
    gkv[:, 0:dim] = key_total.astype(BF16)
    gkv[:, dim:2 * dim] = value_total.astype(BF16)

    def whole(owner, s):
        i = owner * ns + s
        return pre[i] + dot(gkv[...], wkv[pl.ds(pl.multiple_of(i * width, width), width), :], NT)

    def chip_copy(dx, s):
        return remote(tsend.at[dx, s], trcv.at[dx, s], t_send.at[dx, s], t_recv.at[dx, s], heads=other)

    def cross_copy(dx, s):
        return remote(xsend.at[dx, s], xrcv.at[dx, s], x_send.at[dx, s], x_recv.at[dx, s], heads=across[dx])

    order = list(range(1, nx)) + [0]
    for dx in order:
        for s in range(ns):
            tsend[dx, s] = whole(across[dx] + 1 - 2 * core, s).astype(BF16)
            chip_copy(dx, s).start()
        if dx > 0:
            for s in range(ns):
                mine = whole(across[dx], s)
                chip_copy(dx, s).wait_recv()
                xsend[dx, s] = (mine + trcv[dx, s].astype(F32)).astype(BF16)
                cross_copy(dx, s).start()
    for s in range(ns):
        total = whole(h, s)
        chip_copy(0, s).wait_recv()
        total = total + trcv[0, s].astype(F32)
        for dx in range(1, nx):
            cross_copy(dx, s).wait_recv()
            total = total + xrcv[dx, s].astype(F32)
        out_ref[:, s * width:(s + 1) * width] = total.astype(BF16)

    @pl.when(y == 0)
    def _():
        for t in range(2):
            pair_copy(t).wait_send()

    @pl.when(y == 1)
    def _():
        part_copy(z).wait_send()

    def drain(z2, _):
        @pl.when(z2 > z)
        def _():
            for t in range(2):
                own_copy(t, z2).wait_send()

        @pl.when(z2 < z)
        def _():
            for t in range(2):
                relay_copy(t, z2).wait_send()
            part_copy(z2).wait_send()
            fin_copy(z2).wait_send()
        return 0

    lax.fori_loop(0, zs, drain, 0)
    for dx in range(nx):
        for s in range(ns):
            chip_copy(dx, s).wait_send()
            if dx > 0:
                cross_copy(dx, s).wait_send()


def on_device(
    n, nh, queries, key_states, value_states, attention_out, out_grad, log_sum_exp, block_counts,
    w_query, w_key, w_value,
):
    zs, nx, ns = n // 2, nh // 2, 4
    cap, dim = key_states.shape
    width = queries.shape[1]
    rows = width // dim * cap
    model = w_query.shape[0]
    mine = model // nh
    chunk = mine // ns
    vmem = pl.BlockSpec(memory_space=pltpu.VMEM)
    hbm = pl.BlockSpec(memory_space=pl.ANY)
    dma = pltpu.SemaphoreType.DMA
    out, dk, dv = pl.pallas_call(
        functools.partial(kernel, zs, nx, ns),
        out_shape=(
            jax.ShapeDtypeStruct((cap, mine), BF16),
            jax.ShapeDtypeStruct((cap, dim), F32),
            jax.ShapeDtypeStruct((cap, dim), F32),
        ),
        in_specs=[vmem] * 6 + [pl.BlockSpec(memory_space=pltpu.SMEM)] + [hbm] * 3,
        out_specs=(vmem, vmem, vmem),
        scratch_shapes=[
            pltpu.VMEM((model, width), BF16),
            pltpu.VMEM((model, 2 * dim), BF16),
            pltpu.VMEM((rows, dim), BF16),
            pltpu.VMEM((rows, dim), BF16),
            pltpu.VMEM((1, rows), F32),
            pltpu.VMEM((1, rows), F32),
            pltpu.VMEM((dim, rows), F32),
            pltpu.VMEM((cap, width), BF16),
            pltpu.VMEM((cap, 2 * dim), BF16),
            pltpu.VMEM((2, cap, dim), F32),
            pltpu.VMEM((2, n, cap, dim), BF16),
            pltpu.VMEM((zs, 2, cap, dim), F32),
            pltpu.VMEM((zs, 2, cap, dim), BF16),
            pltpu.VMEM((zs, 2, cap, dim), BF16),
            pltpu.VMEM((zs, 2, cap, dim), BF16),
            pltpu.VMEM((zs, 2, cap, dim), BF16),
            pltpu.VMEM((nh * ns, cap, chunk), F32),
            pltpu.VMEM((nx, ns, cap, chunk), BF16),
            pltpu.VMEM((nx, ns, cap, chunk), BF16),
            pltpu.VMEM((nx, ns, cap, chunk), BF16),
            pltpu.VMEM((nx, ns, cap, chunk), BF16),
            dma((3,)),
            dma((2, zs)),
            dma((2,)),
            dma((2, zs)),
            dma((2, n)),
            dma((zs,)),
            dma((zs,)),
            dma((zs,)),
            dma((zs,)),
            dma((nx, ns)),
            dma((nx, ns)),
            dma((nx, ns)),
            dma((nx, ns)),
        ],
        compiler_params=pltpu.CompilerParams(
            collective_id=0, has_side_effects=True, vmem_limit_bytes=52 * 1024 * 1024
        ),
    )(
        queries, key_states, value_states, attention_out, out_grad, log_sum_exp, block_counts,
        w_query, w_key, w_value,
    )
    return out, dk, dv


def solution(mesh):
    return jax.shard_map(
        functools.partial(on_device, mesh.shape["ctx"], mesh.shape["heads"]),
        mesh=mesh,
        in_specs=(
            P("ctx", "heads"),
            P("ctx", "heads"),
            P("ctx", "heads"),
            P("ctx", "heads"),
            P("ctx", "heads"),
            P("heads", "ctx"),
            P(),
            P(None, "heads"),
            P(None, "heads"),
            P(None, "heads"),
        ),
        out_specs=(P("ctx", "heads"), P("ctx", "heads"), P("ctx", "heads")),
        check_vma=False,
    )
```

```python
import functools
import math

import jax
import jax.numpy as jnp
from jax import lax
from jax.experimental import pallas as pl
from jax.experimental.pallas import tpu as pltpu
from jax.sharding import PartitionSpec as P

BLOCK = 64
LOG2E = math.log2(math.e)
F32 = jnp.float32
BF16 = jnp.bfloat16
NT = (((1,), (1,)), ((), ()))
TN = (((0,), (0,)), ((), ()))


def dot(a, b, dims=(((1,), (0,)), ((), ()))):
    return lax.dot_general(a, b, dims, preferred_element_type=F32)


def kernel(
    zs, nx, ns,
    q_hbm, k_hbm, v_hbm, o_hbm, do_hbm, lse_hbm, cnt_ref, wq_hbm, wk_hbm, wv_hbm,
    out_ref, dk_ref, dv_ref,
    q_ref, k_ref, v_ref, o_ref, do_ref, lse_ref, pair_q, pair_do, wq, wkv, qs, dos, lse2, delta, dqt,
    dq_send, dq_recv, gq, gkv, acc, kv, part, fsend, frcv, hold, tsend, trcv, xsend, xrcv,
    in_sem, w_sem, own_send, kv_recv, swap_send, swap_recv, f_send, f_recv,
    t_send, t_recv, x_send, x_recv,
):
    cap, dim = k_ref.shape
    group = q_ref.shape[1] // dim
    scale = 1.0 / math.sqrt(dim)
    me = lax.axis_index("ctx")
    y = lax.rem(me, 2)
    z = lax.div(me, 2)
    pair = me + 1 - 2 * y
    h = lax.axis_index("heads")
    core = lax.rem(h, 2)
    x = lax.div(h, 2)
    other = h + 1 - 2 * core
    across = [2 * lax.rem(x + dx, nx) + core for dx in range(nx)]

    in_copies = [
        pltpu.make_async_copy(src, dst, in_sem.at[i])
        for i, (src, dst) in enumerate((
            (k_hbm, k_ref), (v_hbm, v_ref), (q_hbm, q_ref), (do_hbm, do_ref), (o_hbm, o_ref),
            (lse_hbm, lse_ref),
        ))
    ]
    for copy in in_copies:
        copy.start()
    w_copies = [
        pltpu.make_async_copy(wq_hbm, wq, w_sem.at[0]),
        pltpu.make_async_copy(wk_hbm, wkv.at[:, pl.ds(0, dim)], w_sem.at[1]),
        pltpu.make_async_copy(wv_hbm, wkv.at[:, pl.ds(dim, dim)], w_sem.at[2]),
    ]

    def remote(src, dst, send, recv, **device):
        return pltpu.make_async_remote_copy(
            src_ref=src, dst_ref=dst, send_sem=send, recv_sem=recv,
            device_id=device, device_id_type=pl.DeviceIdType.MESH,
        )

    barrier = pltpu.get_barrier_semaphore()

    def greet(**device):
        pl.semaphore_signal(
            barrier, inc=1, device_id=device, device_id_type=pl.DeviceIdType.MESH
        )

    def greet_line(z2, _):
        @pl.when(z2 != z)
        def _():
            greet(ctx=2 * z2 + y)
        return 0

    lax.fori_loop(0, zs, greet_line, 0)
    greet(ctx=pair)
    greet(heads=other)
    for dx in range(1, nx):
        greet(heads=across[dx])
    for copy in in_copies:
        copy.wait()
    for copy in w_copies:
        copy.start()
    with jax.named_scope("barrier"):
        pl.semaphore_wait(barrier, zs + nx)

    own = (k_ref, v_ref)

    def own_copy(t, z2):
        return remote(own[t], kv.at[t, z], own_send.at[t, z2], kv_recv.at[t, z], ctx=2 * z2 + y)

    def arrived(z1):
        for t in range(2):
            remote(
                kv.at[t, z1], kv.at[t, z1], own_send.at[t, z1], kv_recv.at[t, z1], ctx=pair
            ).wait_recv()

    swaps = [
        remote(src, dst, swap_send.at[i], swap_recv.at[i], ctx=pair)
        for i, (src, dst) in enumerate((
            (q_ref, pair_q), (do_ref, pair_do), (lse2.at[0], lse2.at[1]), (delta.at[0], delta.at[1]),
            (dq_send, dq_recv),
        ))
    ]

    def fin_copy(z1):
        return remote(fsend.at[z1], frcv.at[z], f_send.at[z1], f_recv.at[z], ctx=2 * z1 + y)

    def fin_wait(z2):
        remote(fsend.at[z2], frcv.at[z2], f_send.at[z2], f_recv.at[z2], ctx=2 * z2 + y).wait_recv()

    swaps[0].start()
    swaps[1].start()

    def push_own(i, _):
        z2 = zs - 1 - i

        @pl.when(z2 > z)
        def _():
            for t in range(2):
                own_copy(t, z2).start()
        return 0

    lax.fori_loop(0, zs, push_own, 0)

    lane = lax.broadcasted_iota(jnp.int32, (1, group * cap), 1)
    row = lax.rem(lane, cap)
    alive = row < cnt_ref[me] * BLOCK
    prod = jnp.concatenate(
        [
            do_ref[:, g * dim:(g + 1) * dim].astype(F32) * o_ref[:, g * dim:(g + 1) * dim].astype(F32)
            for g in range(group)
        ],
        axis=0,
    )
    delta[0] = lax.dot_general(
        jnp.ones((8, dim), F32), prod, NT,
        preferred_element_type=F32, precision=lax.Precision.HIGHEST,
    )[0:1]
    lse_row = jnp.concatenate([lse_ref[g:g + 1, :] for g in range(group)], axis=1)
    lse2[0] = jnp.where(alive, lse_row * LOG2E, 1e30)

    def stack(who, q, do):
        for g in range(group):
            cols = slice(g * dim, (g + 1) * dim)
            qs[who, g * cap:(g + 1) * cap, :] = q[:, cols]
            dos[who, g * cap:(g + 1) * cap, :] = do[:, cols]

    stack(0, q_ref, do_ref)
    swaps[2].start()
    swaps[3].start()
    key_row = lax.broadcasted_iota(jnp.int32, (cap, group * cap), 0)

    def tile(who, key, value, b, diagonal):
        scores = dot(key, qs[who], NT)
        prob_grad = dot(value, dos[who], NT)
        visible = key_row < cnt_ref[b] * BLOCK
        if diagonal:
            visible = visible & (key_row <= row)
        prob = jnp.where(visible, jnp.exp2(scores * (scale * LOG2E) - lse2[who]), 0.0)
        grad = (prob * (prob_grad - delta[who])).astype(BF16)
        d_value = dot(prob.astype(BF16), dos[who])
        d_key = dot(grad, qs[who])
        terms = dot(key, grad, TN)
        if diagonal:
            dqt[who] = terms
        else:
            dqt[who] += terms
        return d_key, d_value

    with jax.named_scope("diag"):
        d_key, d_value = tile(0, k_ref[...], v_ref[...], me, True)
        acc[0] = d_key
        acc[1] = d_value
    dqt[1] = jnp.zeros_like(dqt[1])

    def own_step(z1, _):
        @pl.when(z1 < z)
        def _():
            with jax.named_scope("wait_kv"):
                arrived(z1)
            with jax.named_scope("own_tile"):
                d_key, d_value = tile(0, kv[0, z1], kv[1, z1], 2 * z1 + y, False)
                part[z1, 0] = d_key
                part[z1, 1] = d_value
        return 0

    lax.fori_loop(0, zs, own_step, 0)
    with jax.named_scope("wait_swap"):
        for copy in swaps[:4]:
            copy.wait_recv()
    stack(1, pair_q, pair_do)

    def pair_step(z1, _):
        @pl.when(z1 < z)
        def _():
            with jax.named_scope("pair_tile"):
                d_key, d_value = tile(1, kv[0, z1], kv[1, z1], 2 * z1 + y, False)
                fsend[z1, 0] = (part[z1, 0] + d_key).astype(BF16)
                fsend[z1, 1] = (part[z1, 1] + d_value).astype(BF16)
            fin_copy(z1).start()
        return 0

    lax.fori_loop(0, zs, pair_step, 0)

    @pl.when(y == 0)
    def _():
        with jax.named_scope("pair_own"):
            d_key, d_value = tile(1, k_ref[...], v_ref[...], me, False)
            acc[0] += d_key
            acc[1] += d_value

    dq_send[...] = dqt[1].astype(BF16)
    swaps[4].start()

    def collect(i, _):
        z2 = zs - 1 - i

        @pl.when(z2 > z)
        def _():
            fin_wait(z2)
            acc[...] += frcv[z2].astype(F32)
        return 0

    with jax.named_scope("collect"):
        lax.fori_loop(0, zs, collect, 0)
    key_total = acc[0] * scale
    value_total = acc[1]
    dk_ref[...] = key_total
    dv_ref[...] = value_total
    gkv[:, 0:dim] = key_total.astype(BF16)
    gkv[:, dim:2 * dim] = value_total.astype(BF16)
    with jax.named_scope("wait_dq"):
        swaps[4].wait_recv()
    query_grad = (jnp.transpose(dqt[0] + dq_recv[...].astype(F32)) * scale).astype(BF16)
    for g in range(group):
        gq[:, g * dim:(g + 1) * dim] = query_grad[g * cap:(g + 1) * cap, :]
    for copy in w_copies:
        copy.wait()
    width = hold.shape[2]

    def whole(owner, s):
        rows = pl.ds(pl.multiple_of((owner * ns + s) * width, width), width)
        return dot(gq[...], wq[rows, :], NT) + dot(gkv[...], wkv[rows, :], NT)

    def chip_copy(dx, s):
        return remote(tsend.at[dx, s], trcv.at[dx, s], t_send.at[dx, s], t_recv.at[dx, s], heads=other)

    def cross_copy(dx, s):
        return remote(xsend.at[dx, s], xrcv.at[dx, s], x_send.at[dx, s], x_recv.at[dx, s], heads=across[dx])

    def give(dx, s):
        tsend[dx, s] = whole(across[dx] + 1 - 2 * core, s).astype(BF16)
        chip_copy(dx, s).start()

    def cross(dx, s):
        with jax.named_scope("wait_chip"):
            chip_copy(dx, s).wait_recv()
        xsend[dx, s] = (hold[s] + trcv[dx, s].astype(F32)).astype(BF16)
        cross_copy(dx, s).start()

    for dx in range(1, nx):
        for s in range(ns):
            give(dx, s)
            if s > 0:
                cross(dx, s - 1)
            hold[s] = whole(across[dx], s)
        cross(dx, ns - 1)
    for s in range(ns):
        give(0, s)
    for s in range(ns):
        hold[s] = whole(h, s)
    for s in range(ns):
        chip_copy(0, s).wait_recv()
        total = hold[s] + trcv[0, s].astype(F32)
        for dx in range(1, nx):
            with jax.named_scope("wait_cross"):
                cross_copy(dx, s).wait_recv()
            total = total + xrcv[dx, s].astype(F32)
        out_ref[:, s * width:(s + 1) * width] = total.astype(BF16)

    for copy in swaps:
        copy.wait_send()

    def drain(z2, _):
        @pl.when(z2 > z)
        def _():
            for t in range(2):
                own_copy(t, z2).wait_send()

        @pl.when(z2 < z)
        def _():
            fin_copy(z2).wait_send()
        return 0

    lax.fori_loop(0, zs, drain, 0)
    for dx in range(nx):
        for s in range(ns):
            chip_copy(dx, s).wait_send()
            if dx > 0:
                cross_copy(dx, s).wait_send()


def on_device(
    n, nh, queries, key_states, value_states, attention_out, out_grad, log_sum_exp, block_counts,
    w_query, w_key, w_value,
):
    zs, nx, ns = n // 2, nh // 2, 4
    cap, dim = key_states.shape
    width = queries.shape[1]
    rows = width // dim * cap
    model = w_query.shape[0]
    mine = model // nh
    chunk = mine // ns
    vmem = pl.BlockSpec(memory_space=pltpu.VMEM)
    hbm = pl.BlockSpec(memory_space=pl.ANY)
    dma = pltpu.SemaphoreType.DMA
    out, dk, dv = pl.pallas_call(
        functools.partial(kernel, zs, nx, ns),
        out_shape=(
            jax.ShapeDtypeStruct((cap, mine), BF16),
            jax.ShapeDtypeStruct((cap, dim), F32),
            jax.ShapeDtypeStruct((cap, dim), F32),
        ),
        in_specs=[hbm] * 6 + [pl.BlockSpec(memory_space=pltpu.SMEM)] + [hbm] * 3,
        out_specs=(vmem, vmem, vmem),
        scratch_shapes=[
            pltpu.VMEM((cap, width), BF16),
            pltpu.VMEM((cap, dim), BF16),
            pltpu.VMEM((cap, dim), BF16),
            pltpu.VMEM((cap, width), BF16),
            pltpu.VMEM((cap, width), BF16),
            pltpu.VMEM(log_sum_exp.shape, F32),
            pltpu.VMEM((cap, width), BF16),
            pltpu.VMEM((cap, width), BF16),
            pltpu.VMEM((model, width), BF16),
            pltpu.VMEM((model, 2 * dim), BF16),
            pltpu.VMEM((2, rows, dim), BF16),
            pltpu.VMEM((2, rows, dim), BF16),
            pltpu.VMEM((2, 1, rows), F32),
            pltpu.VMEM((2, 1, rows), F32),
            pltpu.VMEM((2, dim, rows), F32),
            pltpu.VMEM((dim, rows), BF16),
            pltpu.VMEM((dim, rows), BF16),
            pltpu.VMEM((cap, width), BF16),
            pltpu.VMEM((cap, 2 * dim), BF16),
            pltpu.VMEM((2, cap, dim), F32),
            pltpu.VMEM((2, zs, cap, dim), BF16),
            pltpu.VMEM((zs, 2, cap, dim), F32),
            pltpu.VMEM((zs, 2, cap, dim), BF16),
            pltpu.VMEM((zs, 2, cap, dim), BF16),
            pltpu.VMEM((ns, cap, chunk), F32),
            pltpu.VMEM((nx, ns, cap, chunk), BF16),
            pltpu.VMEM((nx, ns, cap, chunk), BF16),
            pltpu.VMEM((nx, ns, cap, chunk), BF16),
            pltpu.VMEM((nx, ns, cap, chunk), BF16),
            dma((6,)),
            dma((3,)),
            dma((2, zs)),
            dma((2, zs)),
            dma((5,)),
            dma((5,)),
            dma((zs,)),
            dma((zs,)),
            dma((nx, ns)),
            dma((nx, ns)),
            dma((nx, ns)),
            dma((nx, ns)),
        ],
        compiler_params=pltpu.CompilerParams(
            collective_id=0, has_side_effects=True, vmem_limit_bytes=52 * 1024 * 1024
        ),
    )(
        queries, key_states, value_states, attention_out, out_grad, log_sum_exp, block_counts,
        w_query, w_key, w_value,
    )
    return out, dk, dv


def solution(mesh):
    return jax.shard_map(
        functools.partial(on_device, mesh.shape["ctx"], mesh.shape["heads"]),
        mesh=mesh,
        in_specs=(
            P("ctx", "heads"),
            P("ctx", "heads"),
            P("ctx", "heads"),
            P("ctx", "heads"),
            P("ctx", "heads"),
            P("heads", "ctx"),
            P(),
            P(None, "heads"),
            P(None, "heads"),
            P(None, "heads"),
        ),
        out_specs=(P("ctx", "heads"), P("ctx", "heads"), P("ctx", "heads")),
        check_vma=False,
    )
```

```python
import functools
import math

import jax
import jax.numpy as jnp
from jax import lax
from jax.experimental import pallas as pl
from jax.experimental.pallas import tpu as pltpu
from jax.sharding import PartitionSpec as P

BLOCK = 64
LOG2E = math.log2(math.e)
F32 = jnp.float32
BF16 = jnp.bfloat16
NT = (((1,), (1,)), ((), ()))
TN = (((0,), (0,)), ((), ()))


def dot(a, b, dims=(((1,), (0,)), ((), ()))):
    return lax.dot_general(a, b, dims, preferred_element_type=F32)


def kernel(
    zs, nx, ns,
    q_hbm, k_hbm, v_hbm, o_hbm, do_hbm, lse_hbm, cnt_hbm, wq_hbm, wk_hbm, wv_hbm,
    out_ref, dk_ref, dv_ref,
    cnt_ref, q_ref, k_ref, v_ref, o_ref, do_ref, lse_ref, pair_q, pair_do, wq, wkv, qs, dos, lse2, delta, dqt,
    dq_own, dq_send, dq_recv, gq, gkv, acc, kv, part, fsend, frcv, keep, hold, csend, crcv, tsend, trcv, xsend, xrcv,
    in_sem, w_sem, own_send, kv_recv, swap_send, swap_recv, f_send, f_recv,
    c_send, c_recv, t_send, t_recv, x_send, x_recv,
):
    cap, dim = k_ref.shape
    group = q_ref.shape[1] // dim
    half = cap // 2
    np = cap // half
    scale = 1.0 / math.sqrt(dim)
    me = lax.axis_index("ctx")
    y = lax.rem(me, 2)
    z = lax.div(me, 2)
    pair = me + 1 - 2 * y
    h = lax.axis_index("heads")
    core = lax.rem(h, 2)
    x = lax.div(h, 2)
    other = h + 1 - 2 * core
    across = [2 * lax.rem(x + dx, nx) + core for dx in range(nx)]

    in_copies = [
        pltpu.make_async_copy(src, dst, in_sem.at[i])
        for i, (src, dst) in enumerate((
            (k_hbm, k_ref), (v_hbm, v_ref), (q_hbm, q_ref), (do_hbm, do_ref), (o_hbm, o_ref),
            (lse_hbm, lse_ref), (cnt_hbm, cnt_ref),
        ))
    ]
    for copy in in_copies:
        copy.start()
    w_copies = [
        pltpu.make_async_copy(wq_hbm, wq, w_sem.at[0]),
        pltpu.make_async_copy(wk_hbm, wkv.at[:, pl.ds(0, dim)], w_sem.at[1]),
        pltpu.make_async_copy(wv_hbm, wkv.at[:, pl.ds(dim, dim)], w_sem.at[2]),
    ]

    def remote(src, dst, send, recv, **device):
        return pltpu.make_async_remote_copy(
            src_ref=src, dst_ref=dst, send_sem=send, recv_sem=recv,
            device_id=device, device_id_type=pl.DeviceIdType.MESH,
        )

    barrier = pltpu.get_barrier_semaphore()

    def greet(**device):
        pl.semaphore_signal(
            barrier, inc=1, device_id=device, device_id_type=pl.DeviceIdType.MESH
        )

    def greet_line(z2, _):
        @pl.when(z2 != z)
        def _():
            greet(ctx=2 * z2 + y)
        return 0

    lax.fori_loop(0, zs, greet_line, 0)
    greet(ctx=pair)
    greet(heads=other)
    for dx in range(1, nx):
        greet(heads=across[dx])
    for copy in in_copies:
        copy.wait()
    for copy in w_copies:
        copy.start()
    with jax.named_scope("barrier"):
        pl.semaphore_wait(barrier, zs + nx)

    own = (k_ref, v_ref)

    def own_copy(t, z2):
        return remote(own[t], kv.at[t, z], own_send.at[t, z2], kv_recv.at[t, z], ctx=2 * z2 + y)

    def arrived(z1):
        for t in range(2):
            remote(
                kv.at[t, z1], kv.at[t, z1], own_send.at[t, z1], kv_recv.at[t, z1], ctx=pair
            ).wait_recv()

    swaps = [
        remote(src, dst, swap_send.at[i], swap_recv.at[i], ctx=pair)
        for i, (src, dst) in enumerate((
            (q_ref, pair_q), (do_ref, pair_do), (lse2.at[0], lse2.at[1]), (delta.at[0], delta.at[1]),
            *((dq_send.at[r], dq_recv.at[r]) for r in range(np)),
        ))
    ]

    def fin_copy(r, z1):
        return remote(
            fsend.at[r, z1], frcv.at[r, z], f_send.at[r, z1], f_recv.at[r, z], ctx=2 * z1 + y
        )

    def fin_wait(r, z2):
        remote(
            fsend.at[r, z2], frcv.at[r, z2], f_send.at[r, z2], f_recv.at[r, z2], ctx=2 * z2 + y
        ).wait_recv()

    swaps[0].start()
    swaps[1].start()

    def push_own(i, _):
        z2 = zs - 1 - i

        @pl.when(z2 > z)
        def _():
            for t in range(2):
                own_copy(t, z2).start()
        return 0

    lax.fori_loop(0, zs, push_own, 0)

    lane = lax.broadcasted_iota(jnp.int32, (1, group * cap), 1)
    row = lax.rem(lane, cap)
    alive = row < cnt_ref[me] * BLOCK
    prod = jnp.concatenate(
        [
            do_ref[:, g * dim:(g + 1) * dim].astype(F32) * o_ref[:, g * dim:(g + 1) * dim].astype(F32)
            for g in range(group)
        ],
        axis=0,
    )
    delta[0] = lax.dot_general(
        jnp.ones((8, dim), F32), prod, NT,
        preferred_element_type=F32, precision=lax.Precision.HIGHEST,
    )[0:1]
    lse_row = jnp.concatenate([lse_ref[g:g + 1, :] for g in range(group)], axis=1)
    lse2[0] = jnp.where(alive, lse_row * LOG2E, 1e30)

    def stack(who, q, do):
        for g in range(group):
            cols = slice(g * dim, (g + 1) * dim)
            qs[who, g * cap:(g + 1) * cap, :] = q[:, cols]
            dos[who, g * cap:(g + 1) * cap, :] = do[:, cols]

    stack(0, q_ref, do_ref)
    swaps[2].start()
    swaps[3].start()
    key_row = lax.broadcasted_iota(jnp.int32, (cap, group * cap), 0)

    def tile(who, key, value, b, diagonal):
        scores = dot(key, qs[who], NT)
        prob_grad = dot(value, dos[who], NT)
        visible = key_row < cnt_ref[b] * BLOCK
        if diagonal:
            visible = visible & (key_row <= row)
        prob = jnp.where(visible, jnp.exp2(scores * (scale * LOG2E) - lse2[who]), 0.0)
        grad = (prob * (prob_grad - delta[who])).astype(BF16)
        d_value = dot(prob.astype(BF16), dos[who])
        d_key = dot(grad, qs[who])
        terms = dot(key, grad, TN)
        if diagonal:
            dqt[who] = terms
        else:
            dqt[who] += terms
        return d_key, d_value

    with jax.named_scope("diag"):
        d_key, d_value = tile(0, k_ref[...], v_ref[...], me, True)
        acc[0] = d_key
        acc[1] = d_value
    dqt[1] = jnp.zeros_like(dqt[1])

    def own_step(z1, _):
        @pl.when(z1 < z)
        def _():
            with jax.named_scope("wait_kv"):
                arrived(z1)
            with jax.named_scope("own_tile"):
                d_key, d_value = tile(0, kv[0, z1], kv[1, z1], 2 * z1 + y, False)
                part[z1, 0] = d_key
                part[z1, 1] = d_value
        return 0

    lax.fori_loop(0, zs, own_step, 0)
    with jax.named_scope("wait_swap"):
        for copy in swaps[:4]:
            copy.wait_recv()
    stack(1, pair_q, pair_do)

    def pair_step(z1, _):
        @pl.when(z1 < z)
        def _():
            with jax.named_scope("pair_tile"):
                d_key, d_value = tile(1, kv[0, z1], kv[1, z1], 2 * z1 + y, False)
                d_key = (part[z1, 0] + d_key).astype(BF16)
                d_value = (part[z1, 1] + d_value).astype(BF16)
                for r in range(np):
                    fsend[r, z1, 0] = d_key[r * half:(r + 1) * half]
                    fsend[r, z1, 1] = d_value[r * half:(r + 1) * half]
            fin_copy(0, z1).start()
        return 0

    lax.fori_loop(0, zs, pair_step, 0)

    def later(i, _):
        r = lax.div(i, zs) + 1
        z1 = lax.rem(i, zs)

        @pl.when(z1 < z)
        def _():
            fin_copy(r, z1).start()
        return 0

    lax.fori_loop(0, zs * (np - 1), later, 0)

    @pl.when(y == 0)
    def _():
        with jax.named_scope("pair_own"):
            d_key, d_value = tile(1, k_ref[...], v_ref[...], me, False)
            acc[0] += d_key
            acc[1] += d_value

    pair_dq = jnp.transpose(dqt[1]).astype(BF16)
    for r in range(np):
        for g in range(group):
            dq_send[r, g] = pair_dq[g * cap + r * half:g * cap + (r + 1) * half]
        swaps[4 + r].start()
    dq_own[...] = jnp.transpose(dqt[0])
    for copy in w_copies:
        copy.wait()
    width = hold.shape[2]

    def whole(owner, s, rows):
        cols = pl.ds(pl.multiple_of((owner * ns + s) * width, width), width)
        return dot(gq[rows, :], wq[cols, :], NT) + dot(gkv[rows, :], wkv[cols, :], NT)

    def chip_copy(s):
        return remote(csend.at[s], crcv.at[s], c_send.at[s], c_recv.at[s], heads=other)

    def near_copy(dx, r, s):
        at = (dx, r, s)
        return remote(tsend.at[at], trcv.at[at], t_send.at[at], t_recv.at[at], heads=other)

    def cross_copy(dx, r, s):
        at = (dx, r, s)
        return remote(xsend.at[at], xrcv.at[at], x_send.at[at], x_recv.at[at], heads=across[dx])

    def cross(dx, r, s):
        with jax.named_scope("wait_near"):
            near_copy(dx, r, s).wait_recv()
        xsend[dx, r, s] = (keep[s] + trcv[dx, r, s].astype(F32)).astype(BF16)
        cross_copy(dx, r, s).start()

    for r in range(np):
        rows = slice(r * half, (r + 1) * half)

        def collect(i, _):
            z2 = zs - 1 - i

            @pl.when(z2 > z)
            def _():
                fin_wait(r, z2)
                acc[:, rows, :] += frcv[r, z2].astype(F32)
            return 0

        with jax.named_scope("wait_dq"):
            swaps[4 + r].wait_recv()
        for g in range(group):
            total = dq_own[g * cap + r * half:g * cap + (r + 1) * half, :] + dq_recv[r, g].astype(F32)
            gq[rows, g * dim:(g + 1) * dim] = (total * scale).astype(BF16)
        with jax.named_scope("collect"):
            lax.fori_loop(0, zs, collect, 0)
        key_total = acc[0, rows, :] * scale
        value_total = acc[1, rows, :]
        dk_ref[rows, :] = key_total
        dv_ref[rows, :] = value_total
        gkv[rows, 0:dim] = key_total.astype(BF16)
        gkv[rows, dim:2 * dim] = value_total.astype(BF16)
        for dx in range(1, nx):
            for s in range(ns):
                tsend[dx, r, s] = whole(across[dx] + 1 - 2 * core, s, rows).astype(BF16)
                near_copy(dx, r, s).start()
            for s in range(ns):
                keep[s] = whole(across[dx], s, rows)
                cross(dx, r, s)
    everything = slice(0, cap)
    for s in range(ns):
        csend[s] = whole(other, s, everything).astype(BF16)
        chip_copy(s).start()
    for s in range(ns):
        hold[s] = whole(h, s, everything)
    for s in range(ns):
        chip_copy(s).wait_recv()
        hold[s] += crcv[s].astype(F32)
    for r in range(np):
        rows = slice(r * half, (r + 1) * half)
        for s in range(ns):
            total = hold[s, rows, :]
            for dx in range(1, nx):
                with jax.named_scope("wait_cross"):
                    cross_copy(dx, r, s).wait_recv()
                total = total + xrcv[dx, r, s].astype(F32)
            out_ref[rows, s * width:(s + 1) * width] = total.astype(BF16)

    for copy in swaps:
        copy.wait_send()

    def drain(z2, _):
        @pl.when(z2 > z)
        def _():
            for t in range(2):
                own_copy(t, z2).wait_send()

        @pl.when(z2 < z)
        def _():
            for r in range(np):
                fin_copy(r, z2).wait_send()
        return 0

    lax.fori_loop(0, zs, drain, 0)
    for s in range(ns):
        chip_copy(s).wait_send()
        for dx in range(1, nx):
            for r in range(np):
                near_copy(dx, r, s).wait_send()
                cross_copy(dx, r, s).wait_send()


def on_device(
    n, nh, queries, key_states, value_states, attention_out, out_grad, log_sum_exp, block_counts,
    w_query, w_key, w_value,
):
    zs, nx, ns = n // 2, nh // 2, 4
    cap, dim = key_states.shape
    width = queries.shape[1]
    rows = width // dim * cap
    model = w_query.shape[0]
    mine = model // nh
    chunk = mine // ns
    vmem = pl.BlockSpec(memory_space=pltpu.VMEM)
    half = cap // 2
    np = cap // half
    hbm = pl.BlockSpec(memory_space=pltpu.HBM)
    dma = pltpu.SemaphoreType.DMA
    results = pl.pallas_call(
        functools.partial(kernel, zs, nx, ns),
        out_shape=(
            jax.ShapeDtypeStruct((cap, mine), BF16),
            jax.ShapeDtypeStruct((cap, dim), F32),
            jax.ShapeDtypeStruct((cap, dim), F32),
        ),
        in_specs=[hbm] * 10,
        out_specs=(vmem, vmem, vmem),
        scratch_shapes=[
            pltpu.SMEM(block_counts.shape, jnp.int32),
            pltpu.VMEM((cap, width), BF16),
            pltpu.VMEM((cap, dim), BF16),
            pltpu.VMEM((cap, dim), BF16),
            pltpu.VMEM((cap, width), BF16),
            pltpu.VMEM((cap, width), BF16),
            pltpu.VMEM(log_sum_exp.shape, F32),
            pltpu.VMEM((cap, width), BF16),
            pltpu.VMEM((cap, width), BF16),
            pltpu.VMEM((model, width), BF16),
            pltpu.VMEM((model, 2 * dim), BF16),
            pltpu.VMEM((2, rows, dim), BF16),
            pltpu.VMEM((2, rows, dim), BF16),
            pltpu.VMEM((2, 1, rows), F32),
            pltpu.VMEM((2, 1, rows), F32),
            pltpu.VMEM((2, dim, rows), F32),
            pltpu.VMEM((rows, dim), F32),
            pltpu.VMEM((np, width // dim, half, dim), BF16),
            pltpu.VMEM((np, width // dim, half, dim), BF16),
            pltpu.VMEM((cap, width), BF16),
            pltpu.VMEM((cap, 2 * dim), BF16),
            pltpu.VMEM((2, cap, dim), F32),
            pltpu.VMEM((2, zs, cap, dim), BF16),
            pltpu.VMEM((zs, 2, cap, dim), F32),
            pltpu.VMEM((np, zs, 2, half, dim), BF16),
            pltpu.VMEM((np, zs, 2, half, dim), BF16),
            pltpu.VMEM((ns, half, chunk), F32),
            pltpu.VMEM((ns, cap, chunk), F32),
            pltpu.VMEM((ns, cap, chunk), BF16),
            pltpu.VMEM((ns, cap, chunk), BF16),
            pltpu.VMEM((nx, np, ns, half, chunk), BF16),
            pltpu.VMEM((nx, np, ns, half, chunk), BF16),
            pltpu.VMEM((nx, np, ns, half, chunk), BF16),
            pltpu.VMEM((nx, np, ns, half, chunk), BF16),
            dma((7,)),
            dma((3,)),
            dma((2, zs)),
            dma((2, zs)),
            dma((4 + np,)),
            dma((4 + np,)),
            dma((np, zs)),
            dma((np, zs)),
            dma((ns,)),
            dma((ns,)),
            dma((nx, np, ns)),
            dma((nx, np, ns)),
            dma((nx, np, ns)),
            dma((nx, np, ns)),
        ],
        compiler_params=pltpu.CompilerParams(
            collective_id=0, has_side_effects=True, vmem_limit_bytes=52 * 1024 * 1024
        ),
    )(
        *(
            pltpu.with_memory_space_constraint(a, pltpu.HBM)
            for a in (
                queries, key_states, value_states, attention_out, out_grad, log_sum_exp,
                block_counts, w_query, w_key, w_value,
            )
        )
    )
    return results


def solution(mesh):
    return jax.shard_map(
        functools.partial(on_device, mesh.shape["ctx"], mesh.shape["heads"]),
        mesh=mesh,
        in_specs=(
            P("ctx", "heads"),
            P("ctx", "heads"),
            P("ctx", "heads"),
            P("ctx", "heads"),
            P("ctx", "heads"),
            P("heads", "ctx"),
            P(),
            P(None, "heads"),
            P(None, "heads"),
            P(None, "heads"),
        ),
        out_specs=(P("ctx", "heads"), P("ctx", "heads"), P("ctx", "heads")),
        check_vma=False,
    )
```
